32 devices in a mesh: ga: 8 (over z, core), gp: 4 (over y, x).
Axes of the slice: x: 2, y: 2, z: 4, core: 2. Of those that a mesh axis runs over, the one named last changes fastest.
Arguments:
- matel: bfloat16 [16, 16, 100352], P('ga', None, 'gp'), may hold values from -0.01953125 to 0.01953125
- pole_amp: bfloat16 [1024, 100352], P('ga', 'gp'), may hold values from -6 to 6
- pole_freq: bfloat16 [1024, 100352], P('ga', 'gp'), may hold values from 0.5 to 4
- band_energy: float32 [16], replicated, may hold values from -3 to 3
- energies: float32 [3], replicated, may hold values from -2 to 2
- owner: int32 [5], replicated, may hold values from 0 to 7
- slot: int32 [5], replicated, may hold values from 0 to 1
Outputs:
- sigma: float32 [3, 16, 16], replicated
The draws below stay inside these ranges and needn't reach their ends.
Inputs may be any that keep to these rules, and one draw needn't show every extreme that they name: `slot`: position among the 2 bands stored by that row.
All inputs are finite; a program needn't handle non-finite values.
Results may differ from the reference program's by a relative error of at most 0.0029.
Values may be sent and summed in bfloat16 or wider, within the bound.
No kernel may reach another device: no remote copies, remote signals or barrier semaphores. Data moves between devices by JAX's collectives and lax.ppermute only.
A program may use at most 128 MiB of HBM per device.

```python
import math
import jax
import jax.numpy as jnp
from jax import lax

NG = 100352
TG = 128
NS = 16
HOLD = 2
WIN = 5
NE = 3
RG = 1024
BANDS = 16
N_GA = 8


def touch_ends(values, stream_key, least, largest):
    spot = [jax.random.randint(jax.random.fold_in(stream_key, axis), (), 0, length) for axis, length in enumerate(values.shape)]
    widest = values.shape.index(max(values.shape))
    next_to = spot[:widest] + [(spot[widest] + 1) % values.shape[widest]] + spot[widest + 1:]
    return values.at[tuple(spot)].set(least).at[tuple(next_to)].set(largest)


def block_scale(key, extent, split, low, high):
    def one(position, blocks):
        draws = jax.random.uniform(jax.random.fold_in(jax.random.fold_in(key, 6), position), (blocks,), jnp.float32, low / len(split), high / len(split))
        return jnp.repeat(jnp.exp(draws), extent[position] // blocks).reshape((-1,) + (1,) * (len(extent) - position - 1))

    level = one(*split[0])
    for cut in split[1:]:
        level = level * one(*cut)
    return level


def centred(stream_key, extent, width, reach, pieces=(), held_as=jnp.bfloat16):
    loudness = block_scale(stream_key, extent, pieces, -0.22, 0.18) if pieces else 1.0
    values = jax.random.normal(stream_key, extent, jnp.float32) * width * loudness
    return jnp.minimum(jnp.maximum(values, -reach), reach).astype(held_as)


def setup_inputs(seed: int = 0) -> dict:
    key_list = jax.random.split(jax.random.key(seed), 8)
    return {
        "matel": centred(key_list[0], (BANDS, NS, NG), NG ** -0.5, 0.01953125, ((0, 8), (2, 4))),
        "pole_amp": centred(key_list[1], (RG, NG), 1.0, 6.0, ((0, 8), (1, 4))),
        "pole_freq": jnp.clip(jnp.exp(math.log(4.0) - 2.0794415 * jax.random.uniform(key_list[2], (RG, NG), jnp.float32) ** block_scale(key_list[2], (RG, NG), ((0, 8), (1, 4)), -0.2, 0.2)), 0.5, 4.0).astype(jnp.bfloat16),
        "band_energy": jnp.clip(jax.random.uniform(key_list[3], (BANDS,), jnp.float32, -3.0, 3.0), -3.0, 3.0),
        "energies": jnp.clip(jax.random.uniform(key_list[4], (NE,), jnp.float32, -2.0, 2.0), -2.0, 2.0),
        "owner": touch_ends(jax.random.randint(key_list[5], (WIN,), 0, N_GA), jax.random.fold_in(key_list[5], 1), 0, N_GA - 1).astype(jnp.int32),
        "slot": touch_ends(jax.random.randint(key_list[6], (WIN,), 0, HOLD), jax.random.fold_in(key_list[6], 1), 0, HOLD - 1).astype(jnp.int32),
    }


def reference(matel, pole_amp, pole_freq, band_energy, energies, owner, slot):
    band_index = (owner * HOLD + slot).astype(jnp.int32)
    chosen = matel[band_index]
    levels = band_energy[band_index]
    amp_blocks = pole_amp.reshape(N_GA, TG, NG)
    freq_blocks = pole_freq.reshape(N_GA, TG, NG)
    starts = jnp.arange(N_GA, dtype=jnp.int32) * TG

    def add_block(partial_value, inputs):
        amplitude_block, frequency_block, row_start = inputs
        amplitude = amplitude_block.astype(jnp.float32)
        frequency = frequency_block.astype(jnp.float32)
        numerator = amplitude * frequency
        squared = frequency * frequency
        row_pieces = lax.dynamic_slice_in_dim(chosen, row_start.astype(jnp.int32), TG, 2)
        for band_slot in range(WIN):
            detuning = energies[:, None, None] - levels[band_slot]
            pole_value = (numerator / (detuning * detuning + squared)).astype(jnp.bfloat16)
            pole_value = lax.optimization_barrier(pole_value)
            folded = jnp.einsum("egk,sk->esg", pole_value.astype(jnp.float32), chosen[band_slot].astype(jnp.float32))
            partial_value = partial_value + jnp.einsum("tg,esg->ets", row_pieces[band_slot].astype(jnp.float32), folded, precision=lax.Precision.HIGHEST)
        return partial_value, None

    initial = jnp.zeros((NE, NS, NS), jnp.float32)
    sigma_sum, unused = lax.scan(add_block, initial, (amp_blocks, freq_blocks, starts))
    return sigma_sum
```

```python
import functools

import jax
import jax.numpy as jnp
from jax import lax
from jax.experimental import pallas as pl
from jax.experimental.pallas import tpu as pltpu
from jax.sharding import PartitionSpec as P


def flip(values, axis, size, bit):
    return lax.ppermute(values, axis, [(i, i ^ bit) for i in range(size)])


def tile_width(cols, most):
    best = 128
    for count in range(1, most // 128 + 1):
        if cols % (128 * count) == 0:
            best = 128 * count
    return best


def fold_kernel(detuning_ref, rows_ref, amp_ref, freq_ref, out_ref, *, inner):
    bands = rows_ref.shape[0]
    states = rows_ref.shape[1]
    energies = out_ref.shape[1] // states

    def step(tile, carry):
        columns = pl.ds(pl.multiple_of(tile * inner, inner), inner)
        frequency = freq_ref[:, columns].astype(jnp.float32)
        numerator = amp_ref[:, columns].astype(jnp.float32) * frequency
        squared = frequency * frequency
        for band in range(bands):
            rows = rows_ref[band]
            for energy in range(energies):
                pole = numerator / (squared + detuning_ref[energy, band])
                folded = jnp.dot(rows, pole.astype(jnp.bfloat16), preferred_element_type=jnp.float32)
                out_ref[band, energy * states:(energy + 1) * states, columns] = folded.astype(jnp.bfloat16)
        return carry

    lax.fori_loop(0, amp_ref.shape[1] // inner, step, 0)


def fold(detuning_squared, rows, amp, freq, energies):
    bands, states, depth = rows.shape
    cols = amp.shape[1]
    width = tile_width(cols, 1792)
    inner = 256 if width % 256 == 0 else 128
    return pl.pallas_call(
        functools.partial(fold_kernel, inner=inner),
        grid=(cols // width,),
        in_specs=[
            pl.BlockSpec(memory_space=pltpu.SMEM),
            pl.BlockSpec((bands, states, depth), lambda i: (0, 0, 0)),
            pl.BlockSpec((depth, width), lambda i: (0, i)),
            pl.BlockSpec((depth, width), lambda i: (0, i)),
        ],
        out_specs=pl.BlockSpec((bands, energies * states, width), lambda i: (0, 0, i)),
        out_shape=jax.ShapeDtypeStruct((bands, energies * states, cols), jnp.bfloat16),
        compiler_params=pltpu.CompilerParams(vmem_limit_bytes=32 * 2**20),
        cost_estimate=pl.CostEstimate(
            flops=60 * 10**9, bytes_accessed=26 * 10**6, transcendentals=bands * energies * depth * cols
        ),
        name="fold",
    )(detuning_squared, rows, amp, freq)


def close_kernel(half_ref, column_ref, out_ref):
    @pl.when(pl.program_id(0) == 0)
    def _():
        out_ref[...] = jnp.zeros_like(out_ref)

    total = out_ref[...]
    for band in range(half_ref.shape[0]):
        total += lax.dot_general(
            half_ref[band], column_ref[band], (((1,), (1,)), ((), ())), preferred_element_type=jnp.float32
        )
    out_ref[...] = total


def close(half, column):
    bands, pairs, cols = half.shape
    states = column.shape[1]
    width = tile_width(cols, 3584)
    return pl.pallas_call(
        close_kernel,
        grid=(cols // width,),
        in_specs=[
            pl.BlockSpec((bands, pairs, width), lambda i: (0, 0, i)),
            pl.BlockSpec((bands, states, width), lambda i: (0, 0, i)),
        ],
        out_specs=pl.BlockSpec((pairs, states), lambda i: (0, 0)),
        out_shape=jax.ShapeDtypeStruct((pairs, states), jnp.float32),
        compiler_params=pltpu.CompilerParams(vmem_limit_bytes=32 * 2**20),
        name="close",
    )(half, column)


def held_choice(values, slot):
    picked = values[0]
    for place in range(1, values.shape[0]):
        picked = jnp.where(slot == place, values[place], picked)
    return picked


def shards(matel, pole_amp, pole_freq, band_energy, energies, owner, slot, *, n_ga, n_gp):
    held, states, cols = matel.shape
    depth = pole_amp.shape[0]
    window = owner.shape[0]
    my_row = lax.axis_index("ga")
    my_col = lax.axis_index("gp")

    column = jnp.stack([
        jnp.where(owner[k] == my_row, held_choice(matel, slot[k]), jnp.zeros((), matel.dtype)) for k in range(window)
    ])
    column = lax.psum(column, "ga")

    local = min(cols, n_ga * depth)
    per_block = cols // depth
    pieces = matel[:, :, :local].reshape(held, states, local // depth, depth)
    pieces = jnp.moveaxis(pieces, 2, 0)
    if local < n_ga * depth:
        spare = jnp.zeros((n_ga - local // depth,) + pieces.shape[1:], pieces.dtype)
        pieces = jnp.concatenate([pieces, spare])
        pieces = jnp.roll(pieces, my_col * per_block, axis=0)
    pieces = pieces[:, None]
    bit = n_ga // 2
    mine = my_row
    while bit:
        upper = (mine & bit) != 0
        half = pieces.shape[0] // 2
        keep = jnp.where(upper, pieces[half:], pieces[:half])
        send = jnp.where(upper, pieces[:half], pieces[half:])
        got = flip(send, "ga", n_ga, bit)
        pieces = jnp.where(
            upper, jnp.concatenate([got, keep], axis=1), jnp.concatenate([keep, got], axis=1)
        )
        bit //= 2
    order = pieces[0]
    bits = n_ga.bit_length() - 1
    order = order.reshape((2,) * bits + order.shape[1:])
    order = jnp.transpose(order, tuple(reversed(range(bits))) + tuple(range(bits, order.ndim)))
    order = order.reshape((n_ga * held, states, depth))
    here = my_col == (my_row * depth) // cols
    rows = []
    labels = jnp.arange(n_ga * held, dtype=jnp.int32)
    index = owner * held + slot
    for k in range(window):
        rows.append(lax.dynamic_index_in_dim(order, index[k], 0, keepdims=False))
    rows = jnp.where(here, jnp.stack(rows), jnp.zeros((), matel.dtype))
    bit = 1
    while bit < n_gp:
        rows = rows + flip(rows, "gp", n_gp, bit)
        bit *= 2

    level = jnp.sum(jnp.where(labels[None, :] == index[:, None], band_energy[None, :], 0.0), axis=1)
    detuning = energies[:, None] - level[None, :]
    half = fold(detuning * detuning, rows, pole_amp, pole_freq, energies.shape[0])
    total = close(half, column)

    for axis, size in (("ga", n_ga), ("gp", n_gp)):
        bit = 1
        while bit < size:
            total = total + flip(total, axis, size, bit)
            bit *= 2
    return total.reshape(energies.shape[0], states, states)


def solution(mesh):
    return jax.shard_map(
        functools.partial(shards, n_ga=mesh.shape["ga"], n_gp=mesh.shape["gp"]),
        mesh=mesh,
        in_specs=(P("ga", None, "gp"), P("ga", "gp"), P("ga", "gp"), P(), P(), P(), P()),
        out_specs=P(),
        check_vma=False,
    )
```

```python
import functools

import jax
import jax.numpy as jnp
from jax import lax
from jax.experimental import pallas as pl
from jax.experimental.pallas import tpu as pltpu
from jax.sharding import PartitionSpec as P


FOLD_FLOPS = 48 * 10**9


def flip(values, axis, size, bit):
    return lax.ppermute(values, axis, [(i, i ^ bit) for i in range(size)])


def tile_width(cols, most):
    best = 128
    for count in range(1, most // 128 + 1):
        if cols % (128 * count) == 0:
            best = 128 * count
    return best


def fold_kernel(detuning_ref, rows_ref, amp_ref, freq_ref, out_ref, *, inner):
    bands = rows_ref.shape[0]
    states = rows_ref.shape[1]
    energies = out_ref.shape[1] // states

    def step(tile, carry):
        columns = pl.ds(pl.multiple_of(tile * inner, inner), inner)
        frequency = freq_ref[:, columns].astype(jnp.float32)
        numerator = amp_ref[:, columns].astype(jnp.float32) * frequency
        squared = frequency * frequency
        for band in range(bands):
            rows = rows_ref[band]
            for energy in range(energies):
                pole = numerator / (squared + detuning_ref[energy, band])
                folded = jnp.dot(rows, pole.astype(jnp.bfloat16), preferred_element_type=jnp.float32)
                out_ref[band, energy * states:(energy + 1) * states, columns] = folded.astype(jnp.bfloat16)
        return carry

    lax.fori_loop(0, amp_ref.shape[1] // inner, step, 0)


def fold(detuning_squared, rows, amp, freq, piece, pieces):
    bands, states, depth = rows.shape
    energies = detuning_squared.shape[0]
    cols = amp.shape[1] // pieces
    width = tile_width(cols, 1792)
    steps = cols // width
    inner = 256 if width % 256 == 0 else 128
    return pl.pallas_call(
        functools.partial(fold_kernel, inner=inner),
        grid=(steps,),
        in_specs=[
            pl.BlockSpec(memory_space=pltpu.SMEM),
            pl.BlockSpec((bands, states, depth), lambda i: (0, 0, 0)),
            pl.BlockSpec((depth, width), lambda i: (0, i + piece * steps)),
            pl.BlockSpec((depth, width), lambda i: (0, i + piece * steps)),
        ],
        out_specs=pl.BlockSpec((bands, energies * states, width), lambda i: (0, 0, i)),
        out_shape=jax.ShapeDtypeStruct((bands, energies * states, cols), jnp.bfloat16),
        compiler_params=pltpu.CompilerParams(vmem_limit_bytes=60 * 2**20),
        cost_estimate=pl.CostEstimate(
            flops=FOLD_FLOPS // pieces, bytes_accessed=26 * 10**6 // pieces, transcendentals=0
        ),
        name="fold",
    )(detuning_squared, rows, amp, freq)


def pick_kernel(info_ref, mine_ref, other_ref, first_ref, second_ref, sems, *, base, at, me):
    held = mine_ref.shape[0]
    core = info_ref[me]
    for lane, out_ref in enumerate((first_ref, second_ref)):
        band = info_ref[at + base + lane]
        place = lax.rem(band, held)

        @pl.when(lax.div(band, held) == core)
        def _():
            pltpu.make_async_copy(mine_ref.at[place], out_ref, sems.at[lane]).start()

        @pl.when(lax.div(band, held) != core)
        def _():
            pltpu.make_async_copy(other_ref.at[place], out_ref, sems.at[lane]).start()

    for lane, out_ref in enumerate((first_ref, second_ref)):
        pltpu.make_async_copy(mine_ref.at[0], out_ref, sems.at[lane]).wait()


def pick(info, mine, other, base, at, me):
    shape = jax.ShapeDtypeStruct(mine.shape[1:], mine.dtype)
    return pl.pallas_call(
        functools.partial(pick_kernel, base=base, at=at, me=me),
        in_specs=[
            pl.BlockSpec(memory_space=pltpu.SMEM),
            pl.BlockSpec(memory_space=pltpu.HBM),
            pl.BlockSpec(memory_space=pltpu.HBM),
        ],
        out_specs=[pl.BlockSpec(memory_space=pltpu.VMEM)] * 2,
        out_shape=[shape, shape],
        scratch_shapes=[pltpu.SemaphoreType.DMA((2,))],
        compiler_params=pltpu.CompilerParams(vmem_limit_bytes=60 * 2**20),
        name="pick",
    )(info, mine, other)


def close_kernel(info_ref, *refs, window, pieces, reach, base, at, me):
    halves = refs[:pieces]
    sources = refs[pieces:pieces + 2 + 4 * reach]
    out_ref, half_buf, column_buf, half_sems, column_sems = refs[pieces + 2 + 4 * reach:]
    core = info_ref[me]
    place = info_ref[me + 1]
    sign = 1 - 2 * core
    for band in range(window):
        apart = info_ref[band] - place
        lane = info_ref[window + band] - base
        for which in range(2):
            table = [(sources[which], 0)]
            for hop in range(1, reach + 1):
                table.append((sources[2 + 4 * (hop - 1) + which], sign * hop))
                table.append((sources[4 + 4 * (hop - 1) + which], -sign * hop))
            for ref, distance in table:
                @pl.when((lane == which) & (apart == distance))
                def _():
                    pltpu.make_async_copy(ref, column_buf.at[band], column_sems.at[band]).start()

    for piece in range(pieces):
        pltpu.make_async_copy(halves[piece], half_buf.at[piece], half_sems.at[piece]).start()
    for band in range(window):
        lane = info_ref[window + band] - base
        live = (lane >= 0) & (lane < 2)

        @pl.when(live)
        def _():
            pltpu.make_async_copy(sources[0], column_buf.at[band], column_sems.at[band]).wait()

        @pl.when(jnp.logical_not(live))
        def _():
            column_buf[band] = jnp.zeros_like(column_buf[band])

    width = half_buf.shape[3]

    def step(piece, total):
        pltpu.make_async_copy(halves[0], half_buf.at[piece], half_sems.at[piece]).wait()
        columns = pl.ds(pl.multiple_of(piece * width, 128), width)
        for band in range(window):
            total += lax.dot_general(
                half_buf[piece, band], column_buf[band, :, columns], (((1,), (1,)), ((), ())),
                preferred_element_type=jnp.float32,
            )
        return total

    out_ref[...] = lax.fori_loop(0, pieces, step, jnp.zeros(out_ref.shape, jnp.float32))


def close(info, halves, sources, reach, base, at, me):
    bands, pairs, width = halves[0].shape
    states, cols = sources[0].shape
    pieces = len(halves)
    hbm = pl.BlockSpec(memory_space=pltpu.HBM)
    return pl.pallas_call(
        functools.partial(
            close_kernel, window=bands, pieces=pieces, reach=reach, base=base, at=at, me=me
        ),
        in_specs=[pl.BlockSpec(memory_space=pltpu.SMEM)] + [hbm] * (pieces + len(sources)),
        out_specs=pl.BlockSpec(memory_space=pltpu.VMEM),
        out_shape=jax.ShapeDtypeStruct((pairs, states), jnp.float32),
        scratch_shapes=[
            pltpu.VMEM((pieces, bands, pairs, width), jnp.bfloat16),
            pltpu.VMEM((bands, states, cols), jnp.bfloat16),
            pltpu.SemaphoreType.DMA((pieces,)),
            pltpu.SemaphoreType.DMA((bands,)),
        ],
        compiler_params=pltpu.CompilerParams(vmem_limit_bytes=60 * 2**20),
        name="close",
    )(info, *halves, *sources)


def spread(info, mine, other, base, at, me, n_ga):
    line = [(i + 1, i + 3) for i in range(0, n_ga - 2, 2)] + [(i + 2, i) for i in range(0, n_ga - 2, 2)]
    lanes = list(pick(info, mine, other, base, at, me))
    sources = list(lanes)
    for hop in range(1, n_ga // 2):
        lanes = [lax.ppermute(lane, "ga", line) for lane in lanes]
        sources += lanes
        sources += [flip(lane, "ga", n_ga, 1) for lane in lanes]
    return sources


def row_pieces(matel, index, my_row, my_col, depth, n_ga, n_gp):
    held, states, cols = matel.shape
    local = min(cols, n_ga * depth)
    per_block = cols // depth
    pieces = matel[:, :, :local].reshape(held, states, local // depth, depth)
    pieces = jnp.moveaxis(pieces, 2, 0)
    if local < n_ga * depth:
        spare = jnp.zeros((n_ga - local // depth,) + pieces.shape[1:], pieces.dtype)
        pieces = jnp.concatenate([pieces, spare])
        pieces = jnp.roll(pieces, my_col * per_block, axis=0)
    pieces = pieces[:, None]
    bit = n_ga // 2
    while bit:
        upper = (my_row & bit) != 0
        half = pieces.shape[0] // 2
        keep = jnp.where(upper, pieces[half:], pieces[:half])
        send = jnp.where(upper, pieces[:half], pieces[half:])
        got = flip(send, "ga", n_ga, bit)
        pieces = jnp.where(
            upper, jnp.concatenate([got, keep], axis=1), jnp.concatenate([keep, got], axis=1)
        )
        bit //= 2
    bits = n_ga.bit_length() - 1
    order = pieces[0].reshape((2,) * bits + pieces.shape[2:])
    order = jnp.transpose(order, tuple(reversed(range(bits))) + tuple(range(bits, order.ndim)))
    order = order.reshape((n_ga * held, states, depth))
    here = my_col == (my_row * depth) // cols
    rows = [lax.dynamic_index_in_dim(order, index[k], 0, keepdims=False) for k in range(index.shape[0])]
    rows = jnp.where(here, jnp.stack(rows), jnp.zeros((), matel.dtype))
    bit = 1
    while bit < n_gp:
        rows = rows + flip(rows, "gp", n_gp, bit)
        bit *= 2
    return rows


def shards(matel, pole_amp, pole_freq, band_energy, energies, owner, slot, *, n_ga, n_gp):
    held, states, cols = matel.shape
    depth = pole_amp.shape[0]
    window = owner.shape[0]
    my_row = lax.axis_index("ga")
    my_col = lax.axis_index("gp")
    other = flip(matel, "ga", n_ga, 1)

    chip = owner // 2
    number = (owner % 2) * held + slot
    numbers = jnp.arange(2 * held, dtype=jnp.int32)
    wanted = jnp.any(
        (chip[:, None, None] == chip[None, :, None]) & (number[None, :, None] == numbers), axis=1
    )
    rank = jnp.sum(wanted & (numbers < number[:, None]), axis=1, dtype=jnp.int32)
    on_mine = chip == my_row // 2
    picks = jnp.max(
        jnp.where(on_mine[:, None] & (rank[:, None] == numbers), number[:, None], 0), axis=0
    )
    info = jnp.concatenate([chip, rank, picks, (my_row % 2)[None], (my_row // 2)[None]]).astype(jnp.int32)
    at = 2 * window
    me = at + 2 * held

    sources = spread(info, matel, other, 0, at, me, n_ga)
    index = owner * held + slot
    rows = row_pieces(matel, index, my_row, my_col, depth, n_ga, n_gp)
    labels = jnp.arange(n_ga * held, dtype=jnp.int32)
    level = jnp.sum(jnp.where(labels[None, :] == index[:, None], band_energy[None, :], 0.0), axis=1)
    detuning = energies[:, None] - level[None, :]
    pieces = 7 if cols % (7 * 128) == 0 else 1
    halves = [fold(detuning * detuning, rows, pole_amp, pole_freq, piece, pieces) for piece in range(pieces)]
    reach = n_ga // 2 - 1
    total = close(info, halves, sources, reach, 0, at, me)
    for more in range(1, held):
        def further():
            return close(info, halves, spread(info, matel, other, 2 * more, at, me, n_ga), reach, 2 * more, at, me)

        total = total + lax.cond(jnp.max(rank) >= 2 * more, further, lambda: jnp.zeros_like(total))

    for axis, size in (("ga", n_ga), ("gp", n_gp)):
        bit = 1
        while bit < size:
            total = total + flip(total, axis, size, bit)
            bit *= 2
    return total.reshape(energies.shape[0], states, states)


def solution(mesh):
    return jax.shard_map(
        functools.partial(shards, n_ga=mesh.shape["ga"], n_gp=mesh.shape["gp"]),
        mesh=mesh,
        in_specs=(P("ga", None, "gp"), P("ga", "gp"), P("ga", "gp"), P(), P(), P(), P()),
        out_specs=P(),
        check_vma=False,
    )
```

```python
import functools

import jax
import jax.numpy as jnp
from jax import lax
from jax.experimental import pallas as pl
from jax.experimental.pallas import tpu as pltpu
from jax.sharding import PartitionSpec as P


FOLD_FLOPS = 48 * 10**9


def flip(values, axis, size, bit):
    return lax.ppermute(values, axis, [(i, i ^ bit) for i in range(size)])


def gather_sum(total, axis, size, bit, stop):
    while bit < size and bit <= stop:
        if 2 * bit < size and 2 * bit <= stop:
            parts = [flip(total, axis, size, mask) for mask in (bit, 2 * bit, 3 * bit)]
            total = (total + parts[0]) + (parts[1] + parts[2])
            bit *= 4
        else:
            total = total + flip(total, axis, size, bit)
            bit *= 2
    return total


def tile_width(cols, most):
    best = 128
    for count in range(1, most // 128 + 1):
        if cols % (128 * count) == 0:
            best = 128 * count
    return best


def fold_kernel(index_ref, detuning_ref, rows_ref, amp_ref, freq_ref, out_ref, *, inner):
    bands = out_ref.shape[0]
    states = rows_ref.shape[1]
    energies = out_ref.shape[1] // states

    def step(tile, carry):
        columns = pl.ds(pl.multiple_of(tile * inner, inner), inner)
        frequency = freq_ref[:, columns].astype(jnp.float32)
        numerator = amp_ref[:, columns].astype(jnp.float32) * frequency
        squared = frequency * frequency
        for band in range(bands):
            rows = rows_ref[index_ref[band]]
            for energy in range(energies):
                pole = numerator / (squared + detuning_ref[energy, band])
                folded = jnp.dot(rows, pole.astype(jnp.bfloat16), preferred_element_type=jnp.float32)
                out_ref[band, energy * states:(energy + 1) * states, columns] = folded.astype(jnp.bfloat16)
        return carry

    lax.fori_loop(0, amp_ref.shape[1] // inner, step, 0)


def fold(index, detuning_squared, rows, amp, freq, piece, pieces):
    stored, states, depth = rows.shape
    energies, bands = detuning_squared.shape
    cols = amp.shape[1] // pieces
    width = tile_width(cols, 1792)
    steps = cols // width
    inner = tile_width(width, 896)
    return pl.pallas_call(
        functools.partial(fold_kernel, inner=inner),
        grid=(steps,),
        in_specs=[
            pl.BlockSpec(memory_space=pltpu.SMEM),
            pl.BlockSpec(memory_space=pltpu.SMEM),
            pl.BlockSpec((stored, states, depth), lambda i: (0, 0, 0)),
            pl.BlockSpec((depth, width), lambda i: (0, i + piece * steps)),
            pl.BlockSpec((depth, width), lambda i: (0, i + piece * steps)),
        ],
        out_specs=pl.BlockSpec((bands, energies * states, width), lambda i: (0, 0, i)),
        out_shape=jax.ShapeDtypeStruct((bands, energies * states, cols), jnp.bfloat16),
        compiler_params=pltpu.CompilerParams(vmem_limit_bytes=60 * 2**20),
        cost_estimate=pl.CostEstimate(
            flops=FOLD_FLOPS // pieces, bytes_accessed=26 * 10**6 // pieces, transcendentals=0
        ),
        name="fold",
    )(index, detuning_squared, rows, amp, freq)


def pick_kernel(info_ref, mine_ref, other_ref, first_ref, second_ref, sems, *, base, at, me):
    held = mine_ref.shape[0]
    core = info_ref[me]
    for lane, out_ref in enumerate((first_ref, second_ref)):
        band = info_ref[at + base + lane]
        place = lax.rem(band, held)

        @pl.when(lax.div(band, held) == core)
        def _():
            pltpu.make_async_copy(mine_ref.at[place], out_ref, sems.at[lane]).start()

        @pl.when(lax.div(band, held) != core)
        def _():
            pltpu.make_async_copy(other_ref.at[place], out_ref, sems.at[lane]).start()

    for lane, out_ref in enumerate((first_ref, second_ref)):
        pltpu.make_async_copy(mine_ref.at[0], out_ref, sems.at[lane]).wait()


def pick(info, mine, other, base, at, me):
    shape = jax.ShapeDtypeStruct(mine.shape[1:], mine.dtype)
    return pl.pallas_call(
        functools.partial(pick_kernel, base=base, at=at, me=me),
        in_specs=[
            pl.BlockSpec(memory_space=pltpu.SMEM),
            pl.BlockSpec(memory_space=pltpu.HBM),
            pl.BlockSpec(memory_space=pltpu.HBM),
        ],
        out_specs=[pl.BlockSpec(memory_space=pltpu.VMEM)] * 2,
        out_shape=[shape, shape],
        scratch_shapes=[pltpu.SemaphoreType.DMA((2,))],
        compiler_params=pltpu.CompilerParams(vmem_limit_bytes=60 * 2**20),
        name="pick",
    )(info, mine, other)


def close_kernel(info_ref, *refs, window, pieces, reach, base, at, me):
    halves = refs[:pieces]
    sources = refs[pieces:pieces + 2 + 4 * reach]
    out_ref, half_buf, column_buf, half_sems, column_sems = refs[pieces + 2 + 4 * reach:]
    core = info_ref[me]
    place = info_ref[me + 1]
    sign = 1 - 2 * core
    for band in range(window):
        apart = info_ref[band] - place
        lane = info_ref[window + band] - base
        for which in range(2):
            table = [(sources[which], 0)]
            for hop in range(1, reach + 1):
                table.append((sources[2 + 4 * (hop - 1) + which], sign * hop))
                table.append((sources[4 + 4 * (hop - 1) + which], -sign * hop))
            for ref, distance in table:
                @pl.when((lane == which) & (apart == distance))
                def _():
                    pltpu.make_async_copy(ref, column_buf.at[band], column_sems.at[band]).start()

    for piece in range(pieces):
        pltpu.make_async_copy(halves[piece], half_buf.at[piece], half_sems.at[piece]).start()
    for band in range(window):
        lane = info_ref[window + band] - base
        live = (lane >= 0) & (lane < 2)

        @pl.when(live)
        def _():
            pltpu.make_async_copy(sources[0], column_buf.at[band], column_sems.at[band]).wait()

        @pl.when(jnp.logical_not(live))
        def _():
            column_buf[band] = jnp.zeros_like(column_buf[band])

    width = half_buf.shape[3]

    def step(piece, total):
        pltpu.make_async_copy(halves[0], half_buf.at[piece], half_sems.at[piece]).wait()
        columns = pl.ds(pl.multiple_of(piece * width, 128), width)
        for band in range(window):
            total += lax.dot_general(
                half_buf[piece, band], column_buf[band, :, columns], (((1,), (1,)), ((), ())),
                preferred_element_type=jnp.float32,
            )
        return total

    out_ref[...] = lax.fori_loop(0, pieces, step, jnp.zeros(out_ref.shape, jnp.float32))


def close(info, halves, sources, reach, base, at, me):
    bands, pairs, width = halves[0].shape
    states, cols = sources[0].shape
    pieces = len(halves)
    hbm = pl.BlockSpec(memory_space=pltpu.HBM)
    return pl.pallas_call(
        functools.partial(
            close_kernel, window=bands, pieces=pieces, reach=reach, base=base, at=at, me=me
        ),
        in_specs=[pl.BlockSpec(memory_space=pltpu.SMEM)] + [hbm] * (pieces + len(sources)),
        out_specs=pl.BlockSpec(memory_space=pltpu.VMEM),
        out_shape=jax.ShapeDtypeStruct((pairs, states), jnp.float32),
        scratch_shapes=[
            pltpu.VMEM((pieces, bands, pairs, width), jnp.bfloat16),
            pltpu.VMEM((bands, states, cols), jnp.bfloat16),
            pltpu.SemaphoreType.DMA((pieces,)),
            pltpu.SemaphoreType.DMA((bands,)),
        ],
        compiler_params=pltpu.CompilerParams(vmem_limit_bytes=60 * 2**20),
        name="close",
    )(info, *halves, *sources)


def spread(lanes, n_ga):
    line = [(i + 1, i + 3) for i in range(0, n_ga - 2, 2)] + [(i + 2, i) for i in range(0, n_ga - 2, 2)]
    lanes = list(lanes)
    sources = list(lanes)
    for hop in range(1, n_ga // 2):
        lanes = [lax.ppermute(lane, "ga", line) for lane in lanes]
        sources += lanes
        sources += [flip(lane, "ga", n_ga, 1) for lane in lanes]
    return sources


def row_pieces(matel, lanes, my_row, my_col, depth, n_ga, n_gp):
    held, states, cols = matel.shape
    local = min(cols, n_ga * depth)
    per_block = cols // depth
    pieces = matel[:, :, :local].reshape(held, states, local // depth, depth)
    pieces = jnp.moveaxis(pieces, 2, 0)
    if local < n_ga * depth:
        spare = jnp.zeros((n_ga - local // depth,) + pieces.shape[1:], pieces.dtype)
        pieces = jnp.concatenate([pieces, spare])
        pieces = jnp.roll(pieces, my_col * per_block, axis=0)
    pieces = pieces[:, None]
    bit = n_ga // 2
    while bit:
        upper = (my_row & bit) != 0
        half = pieces.shape[0] // 2
        keep = jnp.where(upper, pieces[half:], pieces[:half])
        send = jnp.where(upper, pieces[:half], pieces[half:])
        got = flip(send, "ga", n_ga, bit)
        pieces = jnp.where(
            upper, jnp.concatenate([got, keep], axis=1), jnp.concatenate([keep, got], axis=1)
        )
        if bit == n_ga // 2:
            pieces, lanes = lax.optimization_barrier((pieces, lanes))
        bit //= 2
    bits = n_ga.bit_length() - 1
    order = pieces[0].reshape((2,) * bits + pieces.shape[2:])
    order = jnp.transpose(order, tuple(reversed(range(bits))) + tuple(range(bits, order.ndim)))
    order = order.reshape((n_ga * held, states, depth))
    here = my_col == (my_row * depth) // cols
    rows = jnp.where(here, order, jnp.zeros((), matel.dtype))
    bit = 1
    while bit < n_gp:
        rows = rows + flip(rows, "gp", n_gp, bit)
        bit *= 2
    return rows, lanes


def shards(matel, pole_amp, pole_freq, band_energy, energies, owner, slot, *, n_ga, n_gp):
    held, states, cols = matel.shape
    depth = pole_amp.shape[0]
    window = owner.shape[0]
    my_row = lax.axis_index("ga")
    my_col = lax.axis_index("gp")
    other = flip(matel, "ga", n_ga, 1)

    chip = owner // 2
    number = (owner % 2) * held + slot
    numbers = jnp.arange(2 * held, dtype=jnp.int32)
    wanted = jnp.any(
        (chip[:, None, None] == chip[None, :, None]) & (number[None, :, None] == numbers), axis=1
    )
    rank = jnp.sum(wanted & (numbers < number[:, None]), axis=1, dtype=jnp.int32)
    on_mine = chip == my_row // 2
    picks = jnp.max(
        jnp.where(on_mine[:, None] & (rank[:, None] == numbers), number[:, None], 0), axis=0
    )
    info = jnp.concatenate([chip, rank, picks, (my_row % 2)[None], (my_row // 2)[None]]).astype(jnp.int32)
    at = 2 * window
    me = at + 2 * held

    index = owner * held + slot
    rows, lanes = row_pieces(matel, pick(info, matel, other, 0, at, me), my_row, my_col, depth, n_ga, n_gp)
    sources = spread(lanes, n_ga)
    labels = jnp.arange(n_ga * held, dtype=jnp.int32)
    level = jnp.sum(jnp.where(labels[None, :] == index[:, None], band_energy[None, :], 0.0), axis=1)
    detuning = energies[:, None] - level[None, :]
    pieces = 7 if cols % (7 * 128) == 0 else 1
    halves = [fold(index, detuning * detuning, rows, pole_amp, pole_freq, piece, pieces) for piece in range(pieces)]
    reach = n_ga // 2 - 1
    total = close(info, halves, sources, reach, 0, at, me)
    for more in range(1, held):
        def further():
            return close(info, halves, spread(pick(info, matel, other, 2 * more, at, me), n_ga), reach, 2 * more, at, me)

        total = total + lax.cond(jnp.max(rank) >= 2 * more, further, lambda: jnp.zeros_like(total))

    total = gather_sum(total, "ga", n_ga, 1, 1)
    total = gather_sum(total, "ga", n_ga, 2, n_ga)
    total = gather_sum(total, "gp", n_gp, 1, n_gp)
    return total.reshape(energies.shape[0], states, states)


def solution(mesh):
    return jax.shard_map(
        functools.partial(shards, n_ga=mesh.shape["ga"], n_gp=mesh.shape["gp"]),
        mesh=mesh,
        in_specs=(P("ga", None, "gp"), P("ga", "gp"), P("ga", "gp"), P(), P(), P(), P()),
        out_specs=P(),
        check_vma=False,
    )
```

```python
import functools

import jax
import jax.numpy as jnp
from jax import lax
from jax.experimental import pallas as pl
from jax.experimental.pallas import tpu as pltpu
from jax.sharding import PartitionSpec as P


FOLD_FLOPS = 48 * 10**9


def flip(values, axis, size, bit):
    return lax.ppermute(values, axis, [(i, i ^ bit) for i in range(size)])


def gather_sum(total, axis, size, bit, stop):
    while bit < size and bit <= stop:
        if 2 * bit < size and 2 * bit <= stop:
            parts = [flip(total, axis, size, mask) for mask in (bit, 2 * bit, 3 * bit)]
            total = (total + parts[0]) + (parts[1] + parts[2])
            bit *= 4
        else:
            total = total + flip(total, axis, size, bit)
            bit *= 2
    return total


def tile_width(cols, most):
    best = 128
    for count in range(1, most // 128 + 1):
        if cols % (128 * count) == 0:
            best = 128 * count
    return best


def fold_kernel(index_ref, detuning_ref, rows_ref, amp_ref, freq_ref, out_ref, *, inner):
    bands = out_ref.shape[0]
    states = rows_ref.shape[1]
    energies = out_ref.shape[1] // states

    def step(tile, carry):
        columns = pl.ds(pl.multiple_of(tile * inner, inner), inner)
        frequency = freq_ref[:, columns].astype(jnp.float32)
        numerator = amp_ref[:, columns].astype(jnp.float32) * frequency
        squared = frequency * frequency
        for band in range(bands):
            rows = rows_ref[index_ref[band]]
            for energy in range(energies):
                pole = numerator / (squared + detuning_ref[energy, band])
                folded = jnp.dot(rows, pole.astype(jnp.bfloat16), preferred_element_type=jnp.float32)
                out_ref[band, energy * states:(energy + 1) * states, columns] = folded.astype(jnp.bfloat16)
        return carry

    lax.fori_loop(0, amp_ref.shape[1] // inner, step, 0)


def fold(index, detuning_squared, rows, amp, freq, piece):
    stored, states, depth = rows.shape
    energies, bands = detuning_squared.shape
    width = tile_width(amp.shape[1], 1792)
    first, steps = piece
    cols = steps * width
    inner = tile_width(width, 896)
    return pl.pallas_call(
        functools.partial(fold_kernel, inner=inner),
        grid=(steps,),
        in_specs=[
            pl.BlockSpec(memory_space=pltpu.SMEM),
            pl.BlockSpec(memory_space=pltpu.SMEM),
            pl.BlockSpec((stored, states, depth), lambda i: (0, 0, 0)),
            pl.BlockSpec((depth, width), lambda i: (0, i + first)),
            pl.BlockSpec((depth, width), lambda i: (0, i + first)),
        ],
        out_specs=pl.BlockSpec((bands, energies * states, width), lambda i: (0, 0, i)),
        out_shape=jax.ShapeDtypeStruct((bands, energies * states, cols), jnp.bfloat16),
        compiler_params=pltpu.CompilerParams(vmem_limit_bytes=60 * 2**20),
        cost_estimate=pl.CostEstimate(
            flops=FOLD_FLOPS * cols // amp.shape[1], bytes_accessed=2 * depth * cols, transcendentals=0
        ),
        name="fold",
    )(index, detuning_squared, rows, amp, freq)


def pick_kernel(info_ref, mine_ref, other_ref, first_ref, second_ref, sems, *, base, at, me):
    held = mine_ref.shape[0]
    core = info_ref[me]
    for lane, out_ref in enumerate((first_ref, second_ref)):
        band = info_ref[at + base + lane]
        place = lax.rem(band, held)

        @pl.when(lax.div(band, held) == core)
        def _():
            pltpu.make_async_copy(mine_ref.at[place], out_ref, sems.at[lane]).start()

        @pl.when(lax.div(band, held) != core)
        def _():
            pltpu.make_async_copy(other_ref.at[place], out_ref, sems.at[lane]).start()

    for lane, out_ref in enumerate((first_ref, second_ref)):
        pltpu.make_async_copy(mine_ref.at[0], out_ref, sems.at[lane]).wait()


def pick(info, mine, other, base, at, me):
    shape = jax.ShapeDtypeStruct(mine.shape[1:], mine.dtype)
    return pl.pallas_call(
        functools.partial(pick_kernel, base=base, at=at, me=me),
        in_specs=[
            pl.BlockSpec(memory_space=pltpu.SMEM),
            pl.BlockSpec(memory_space=pltpu.HBM),
            pl.BlockSpec(memory_space=pltpu.HBM),
        ],
        out_specs=[pl.BlockSpec(memory_space=pltpu.VMEM)] * 2,
        out_shape=[shape, shape],
        scratch_shapes=[pltpu.SemaphoreType.DMA((2,))],
        compiler_params=pltpu.CompilerParams(vmem_limit_bytes=60 * 2**20),
        name="pick",
    )(info, mine, other)


def close_kernel(info_ref, *refs, window, pieces, reach, unit, base, at, me):
    halves = refs[:pieces]
    sources = refs[pieces:pieces + 2 + 4 * reach]
    out_ref, half_buf, column_buf, half_sems, column_sems = refs[pieces + 2 + 4 * reach:]
    core = info_ref[me]
    place = info_ref[me + 1]
    sign = 1 - 2 * core
    for band in range(window):
        apart = info_ref[band] - place
        lane = info_ref[window + band] - base
        for which in range(2):
            table = [(sources[which], 0)]
            for hop in range(1, reach + 1):
                table.append((sources[2 + 4 * (hop - 1) + which], sign * hop))
                table.append((sources[4 + 4 * (hop - 1) + which], -sign * hop))
            for ref, distance in table:
                @pl.when((lane == which) & (apart == distance))
                def _():
                    pltpu.make_async_copy(ref, column_buf.at[band], column_sems.at[band]).start()

    width = unit
    starts = []
    for half in halves:
        for part in range(half.shape[2] // width):
            place_in = pl.ds(part * width, width)
            pltpu.make_async_copy(half.at[:, :, place_in], half_buf.at[len(starts)], half_sems.at[len(starts)]).start()
            starts.append(part)
    for band in range(window):
        lane = info_ref[window + band] - base
        live = (lane >= 0) & (lane < 2)

        @pl.when(live)
        def _():
            pltpu.make_async_copy(sources[0], column_buf.at[band], column_sems.at[band]).wait()

        @pl.when(jnp.logical_not(live))
        def _():
            column_buf[band] = jnp.zeros_like(column_buf[band])

    def step(piece, total):
        pltpu.make_async_copy(halves[0].at[:, :, pl.ds(0, width)], half_buf.at[piece], half_sems.at[piece]).wait()
        columns = pl.ds(pl.multiple_of(piece * width, 128), width)
        for band in range(window):
            total += lax.dot_general(
                half_buf[piece, band], column_buf[band, :, columns], (((1,), (1,)), ((), ())),
                preferred_element_type=jnp.float32,
            )
        return total

    out_ref[...] = lax.fori_loop(0, len(starts), step, jnp.zeros(out_ref.shape, jnp.float32))


def close(info, halves, sources, reach, base, at, me):
    bands, pairs = halves[0].shape[:2]
    states, cols = sources[0].shape
    pieces = len(halves)
    unit = tile_width(cols, 1792)
    hbm = pl.BlockSpec(memory_space=pltpu.HBM)
    return pl.pallas_call(
        functools.partial(
            close_kernel, window=bands, pieces=pieces, reach=reach, unit=unit, base=base, at=at, me=me
        ),
        in_specs=[pl.BlockSpec(memory_space=pltpu.SMEM)] + [hbm] * (pieces + len(sources)),
        out_specs=pl.BlockSpec(memory_space=pltpu.VMEM),
        out_shape=jax.ShapeDtypeStruct((pairs, states), jnp.float32),
        scratch_shapes=[
            pltpu.VMEM((cols // unit, bands, pairs, unit), jnp.bfloat16),
            pltpu.VMEM((bands, states, cols), jnp.bfloat16),
            pltpu.SemaphoreType.DMA((cols // unit,)),
            pltpu.SemaphoreType.DMA((bands,)),
        ],
        compiler_params=pltpu.CompilerParams(vmem_limit_bytes=60 * 2**20),
        name="close",
    )(info, *halves, *sources)


def spread(lanes, n_ga):
    line = [(i + 1, i + 3) for i in range(0, n_ga - 2, 2)] + [(i + 2, i) for i in range(0, n_ga - 2, 2)]
    lanes = list(lanes)
    sources = list(lanes)
    for _ in range(1, n_ga // 2):
        hopped = []
        for lane in lanes:
            hopped.append(lax.ppermute(lane, "ga", line))
        lanes = hopped
        sources += lanes
        sources += [flip(lane, "ga", n_ga, 1) for lane in lanes]
    return sources


def row_pieces(matel, lanes, my_row, my_col, depth, n_ga, n_gp):
    held, states, cols = matel.shape
    local = min(cols, n_ga * depth)
    per_block = cols // depth
    pieces = matel[:, :, :local].reshape(held, states, local // depth, depth)
    pieces = jnp.moveaxis(pieces, 2, 0)
    if local < n_ga * depth:
        spare = jnp.zeros((n_ga - local // depth,) + pieces.shape[1:], pieces.dtype)
        pieces = jnp.concatenate([pieces, spare])
        pieces = jnp.roll(pieces, my_col * per_block, axis=0)
    pieces = pieces[:, None]
    bit = n_ga // 2
    while bit:
        upper = (my_row & bit) != 0
        half = pieces.shape[0] // 2
        keep = jnp.where(upper, pieces[half:], pieces[:half])
        send = jnp.where(upper, pieces[:half], pieces[half:])
        got = flip(send, "ga", n_ga, bit)
        pieces = jnp.where(
            upper, jnp.concatenate([got, keep], axis=1), jnp.concatenate([keep, got], axis=1)
        )
        if bit == n_ga // 2:
            pieces, lanes = lax.optimization_barrier((pieces, lanes))
        bit //= 2
    bits = n_ga.bit_length() - 1
    order = pieces[0].reshape((2,) * bits + pieces.shape[2:])
    order = jnp.transpose(order, tuple(reversed(range(bits))) + tuple(range(bits, order.ndim)))
    order = order.reshape((n_ga * held, states, depth))
    here = my_col == (my_row * depth) // cols
    rows = jnp.where(here, order, jnp.zeros((), matel.dtype))
    bit = 1
    while bit < n_gp:
        rows = rows + flip(rows, "gp", n_gp, bit)
        bit *= 2
    return rows, lanes


def shards(matel, pole_amp, pole_freq, band_energy, energies, owner, slot, *, n_ga, n_gp):
    held, states, cols = matel.shape
    depth = pole_amp.shape[0]
    window = owner.shape[0]
    my_row = lax.axis_index("ga")
    my_col = lax.axis_index("gp")
    other = flip(matel, "ga", n_ga, 1)

    chip = owner // 2
    number = (owner % 2) * held + slot
    numbers = jnp.arange(2 * held, dtype=jnp.int32)
    wanted = jnp.any(
        (chip[:, None, None] == chip[None, :, None]) & (number[None, :, None] == numbers), axis=1
    )
    rank = jnp.sum(wanted & (numbers < number[:, None]), axis=1, dtype=jnp.int32)
    on_mine = chip == my_row // 2
    picks = jnp.max(
        jnp.where(on_mine[:, None] & (rank[:, None] == numbers), number[:, None], 0), axis=0
    )
    info = jnp.concatenate([chip, rank, picks, (my_row % 2)[None], (my_row // 2)[None]]).astype(jnp.int32)
    at = 2 * window
    me = at + 2 * held

    index = owner * held + slot
    rows, lanes = row_pieces(matel, pick(info, matel, other, 0, at, me), my_row, my_col, depth, n_ga, n_gp)
    sources = spread(lanes, n_ga)
    labels = jnp.arange(n_ga * held, dtype=jnp.int32)
    level = jnp.sum(jnp.where(labels[None, :] == index[:, None], band_energy[None, :], 0.0), axis=1)
    detuning = energies[:, None] - level[None, :]
    blocks = cols // tile_width(cols, 1792)
    early = max(1, blocks // 7)
    middle = (blocks - early) // 2
    halves = []
    for number, piece in enumerate(((0, early), (early, middle), (early + middle, blocks - early - middle))):
        halves.append(fold(index, detuning * detuning, rows, pole_amp, pole_freq, piece))
    reach = n_ga // 2 - 1
    total = close(info, halves, sources, reach, 0, at, me)
    for more in range(1, held):
        def further(total):
            sources = spread(pick(info, matel, other, 2 * more, at, me), n_ga)
            return total + close(info, halves, sources, reach, 2 * more, at, me)

        total = lax.cond(jnp.max(rank) >= 2 * more, further, lambda total: total, total)

    total = gather_sum(total, "ga", n_ga, 1, 1)
    total = gather_sum(total, "ga", n_ga, 2, n_ga)
    total = gather_sum(total, "gp", n_gp, 1, n_gp)
    return total.reshape(energies.shape[0], states, states)


def solution(mesh):
    n_ga, n_gp = mesh.shape["ga"], mesh.shape["gp"]

    def body(*values):
        return shards(*values, n_ga=n_ga, n_gp=n_gp)

    return jax.shard_map(
        body,
        mesh=mesh,
        in_specs=(P("ga", None, "gp"), P("ga", "gp"), P("ga", "gp"), P(), P(), P(), P()),
        out_specs=P(),
        check_vma=False,
    )
```

```python
import functools

import jax
import jax.numpy as jnp
from jax import lax
from jax.experimental import pallas as pl
from jax.experimental.pallas import tpu as pltpu
from jax.sharding import PartitionSpec as P


FOLD_FLOPS = 48 * 10**9


def flip(values, axis, size, bit):
    return lax.ppermute(values, axis, [(i, i ^ bit) for i in range(size)])


def gather_sum(total, axis, size, bit, stop):
    while bit < size and bit <= stop:
        if 2 * bit < size and 2 * bit <= stop:
            parts = [flip(total, axis, size, mask) for mask in (bit, 2 * bit, 3 * bit)]
            total = (total + parts[0]) + (parts[1] + parts[2])
            bit *= 4
        else:
            total = total + flip(total, axis, size, bit)
            bit *= 2
    return total


def tile_width(cols, most):
    best = 128
    for count in range(1, most // 128 + 1):
        if cols % (128 * count) == 0:
            best = 128 * count
    return best


def fold_kernel(index_ref, detuning_ref, rows_ref, amp_ref, freq_ref, out_ref, *, inner):
    bands = out_ref.shape[0]
    states = rows_ref.shape[1]
    energies = out_ref.shape[1] // states

    def step(tile, carry):
        columns = pl.ds(pl.multiple_of(tile * inner, inner), inner)
        frequency = freq_ref[:, columns].astype(jnp.float32)
        numerator = amp_ref[:, columns].astype(jnp.float32) * frequency
        squared = frequency * frequency
        for band in range(bands):
            rows = rows_ref[index_ref[band]]
            for energy in range(energies):
                pole = numerator / (squared + detuning_ref[energy, band])
                folded = jnp.dot(rows, pole.astype(jnp.bfloat16), preferred_element_type=jnp.float32)
                out_ref[band, energy * states:(energy + 1) * states, columns] = folded.astype(jnp.bfloat16)
        return carry

    lax.fori_loop(0, amp_ref.shape[1] // inner, step, 0)


def fold(index, detuning_squared, rows, amp, freq, piece):
    stored, states, depth = rows.shape
    energies, bands = detuning_squared.shape
    width = tile_width(amp.shape[1], 1792)
    first, steps = piece
    cols = steps * width
    inner = tile_width(width, 896)
    return pl.pallas_call(
        functools.partial(fold_kernel, inner=inner),
        grid=(steps,),
        in_specs=[
            pl.BlockSpec(memory_space=pltpu.SMEM),
            pl.BlockSpec(memory_space=pltpu.SMEM),
            pl.BlockSpec((stored, states, depth), lambda i: (0, 0, 0)),
            pl.BlockSpec((depth, width), lambda i: (0, i + first)),
            pl.BlockSpec((depth, width), lambda i: (0, i + first)),
        ],
        out_specs=pl.BlockSpec((bands, energies * states, width), lambda i: (0, 0, i)),
        out_shape=jax.ShapeDtypeStruct((bands, energies * states, cols), jnp.bfloat16),
        compiler_params=pltpu.CompilerParams(vmem_limit_bytes=60 * 2**20),
        cost_estimate=pl.CostEstimate(
            flops=FOLD_FLOPS * cols // amp.shape[1], bytes_accessed=2 * depth * cols, transcendentals=0
        ),
        name="fold",
    )(index, detuning_squared, rows, amp, freq)


def pick_kernel(info_ref, mine_ref, other_ref, first_ref, second_ref, sems, *, base, at, me):
    held = mine_ref.shape[0]
    core = info_ref[me]
    for lane, out_ref in enumerate((first_ref, second_ref)):
        band = info_ref[at + base + lane]
        place = lax.rem(band, held)

        @pl.when(lax.div(band, held) == core)
        def _():
            pltpu.make_async_copy(mine_ref.at[place], out_ref, sems.at[lane]).start()

        @pl.when(lax.div(band, held) != core)
        def _():
            pltpu.make_async_copy(other_ref.at[place], out_ref, sems.at[lane]).start()

    for lane, out_ref in enumerate((first_ref, second_ref)):
        pltpu.make_async_copy(mine_ref.at[0], out_ref, sems.at[lane]).wait()


def pick(info, mine, other, base, at, me):
    shape = jax.ShapeDtypeStruct(mine.shape[1:], mine.dtype)
    return pl.pallas_call(
        functools.partial(pick_kernel, base=base, at=at, me=me),
        in_specs=[
            pl.BlockSpec(memory_space=pltpu.SMEM),
            pl.BlockSpec(memory_space=pltpu.HBM),
            pl.BlockSpec(memory_space=pltpu.HBM),
        ],
        out_specs=[pl.BlockSpec(memory_space=pltpu.VMEM)] * 2,
        out_shape=[shape, shape],
        scratch_shapes=[pltpu.SemaphoreType.DMA((2,))],
        compiler_params=pltpu.CompilerParams(vmem_limit_bytes=60 * 2**20),
        name="pick",
    )(info, mine, other)


def close_kernel(info_ref, *refs, window, pieces, reach, unit, base, at, me):
    halves = refs[:pieces]
    sources = refs[pieces:pieces + 2 + 4 * reach]
    out_ref, half_buf, column_buf, half_sems, column_sems = refs[pieces + 2 + 4 * reach:]
    core = info_ref[me]
    place = info_ref[me + 1]
    sign = 1 - 2 * core
    for band in range(window):
        apart = info_ref[band] - place
        lane = info_ref[window + band] - base
        for which in range(2):
            table = [(sources[which], 0)]
            for hop in range(1, reach + 1):
                table.append((sources[2 + 4 * (hop - 1) + which], sign * hop))
                table.append((sources[4 + 4 * (hop - 1) + which], -sign * hop))
            for ref, distance in table:
                @pl.when((lane == which) & (apart == distance))
                def _():
                    pltpu.make_async_copy(ref, column_buf.at[band], column_sems.at[band]).start()

    width = unit
    starts = []
    for half in halves:
        for part in range(half.shape[2] // width):
            place_in = pl.ds(part * width, width)
            pltpu.make_async_copy(half.at[:, :, place_in], half_buf.at[len(starts)], half_sems.at[len(starts)]).start()
            starts.append(part)
    for band in range(window):
        lane = info_ref[window + band] - base
        live = (lane >= 0) & (lane < 2)

        @pl.when(live)
        def _():
            pltpu.make_async_copy(sources[0], column_buf.at[band], column_sems.at[band]).wait()

        @pl.when(jnp.logical_not(live))
        def _():
            column_buf[band] = jnp.zeros_like(column_buf[band])

    def step(piece, total):
        pltpu.make_async_copy(halves[0].at[:, :, pl.ds(0, width)], half_buf.at[piece], half_sems.at[piece]).wait()
        columns = pl.ds(pl.multiple_of(piece * width, 128), width)
        for band in range(window):
            total += lax.dot_general(
                half_buf[piece, band], column_buf[band, :, columns], (((1,), (1,)), ((), ())),
                preferred_element_type=jnp.float32,
            )
        return total

    out_ref[...] = lax.fori_loop(0, len(starts), step, jnp.zeros(out_ref.shape, jnp.float32))


def close(info, halves, sources, reach, base, at, me):
    bands, pairs = halves[0].shape[:2]
    states, cols = sources[0].shape
    pieces = len(halves)
    unit = tile_width(cols, 1792)
    hbm = pl.BlockSpec(memory_space=pltpu.HBM)
    return pl.pallas_call(
        functools.partial(
            close_kernel, window=bands, pieces=pieces, reach=reach, unit=unit, base=base, at=at, me=me
        ),
        in_specs=[pl.BlockSpec(memory_space=pltpu.SMEM)] + [hbm] * (pieces + len(sources)),
        out_specs=pl.BlockSpec(memory_space=pltpu.VMEM),
        out_shape=jax.ShapeDtypeStruct((pairs, states), jnp.float32),
        scratch_shapes=[
            pltpu.VMEM((cols // unit, bands, pairs, unit), jnp.bfloat16),
            pltpu.VMEM((bands, states, cols), jnp.bfloat16),
            pltpu.SemaphoreType.DMA((cols // unit,)),
            pltpu.SemaphoreType.DMA((bands,)),
        ],
        compiler_params=pltpu.CompilerParams(vmem_limit_bytes=60 * 2**20),
        name="close",
    )(info, *halves, *sources)


def spread(lanes, n_ga):
    line = [(i + 1, i + 3) for i in range(0, n_ga - 2, 2)] + [(i + 2, i) for i in range(0, n_ga - 2, 2)]
    lanes = list(lanes)
    sources = list(lanes)
    for _ in range(1, n_ga // 2):
        hopped = []
        for lane in lanes:
            hopped.append(lax.ppermute(lane, "ga", line))
        lanes = hopped
        sources += lanes
        for lane in lanes:
            sources.append(flip(lane, "ga", n_ga, 1))
    return sources


def row_pieces(matel, lanes, my_row, my_col, depth, n_ga, n_gp):
    held, states, cols = matel.shape
    local = min(cols, n_ga * depth)
    per_block = cols // depth
    pieces = matel[:, :, :local].reshape(held, states, local // depth, depth)
    pieces = jnp.moveaxis(pieces, 2, 0)
    if local < n_ga * depth:
        spare = jnp.zeros((n_ga - local // depth,) + pieces.shape[1:], pieces.dtype)
        pieces = jnp.concatenate([pieces, spare])
        pieces = jnp.roll(pieces, my_col * per_block, axis=0)
    pieces = pieces[:, None]
    bit = n_ga // 2
    while bit:
        upper = (my_row & bit) != 0
        half = pieces.shape[0] // 2
        keep = jnp.where(upper, pieces[half:], pieces[:half])
        send = jnp.where(upper, pieces[:half], pieces[half:])
        got = flip(send, "ga", n_ga, bit)
        pieces = jnp.where(
            upper, jnp.concatenate([got, keep], axis=1), jnp.concatenate([keep, got], axis=1)
        )
        if bit == min(2, n_ga // 2):
            pieces, lanes = lax.optimization_barrier((pieces, lanes))
        bit //= 2
    bits = n_ga.bit_length() - 1
    order = pieces[0].reshape((2,) * bits + pieces.shape[2:])
    order = jnp.transpose(order, tuple(reversed(range(bits))) + tuple(range(bits, order.ndim)))
    order = order.reshape((n_ga * held, states, depth))
    here = my_col == (my_row * depth) // cols
    rows = jnp.where(here, order, jnp.zeros((), matel.dtype))
    bit = 1
    while bit < n_gp:
        rows = rows + flip(rows, "gp", n_gp, bit)
        bit *= 2
    return rows, lanes


def shards(matel, pole_amp, pole_freq, band_energy, energies, owner, slot, *, n_ga, n_gp):
    held, states, cols = matel.shape
    depth = pole_amp.shape[0]
    window = owner.shape[0]
    my_row = lax.axis_index("ga")
    my_col = lax.axis_index("gp")
    other = flip(matel, "ga", n_ga, 1)

    chip = owner // 2
    number = (owner % 2) * held + slot
    numbers = jnp.arange(2 * held, dtype=jnp.int32)
    wanted = jnp.any(
        (chip[:, None, None] == chip[None, :, None]) & (number[None, :, None] == numbers), axis=1
    )
    rank = jnp.sum(wanted & (numbers < number[:, None]), axis=1, dtype=jnp.int32)
    on_mine = chip == my_row // 2
    picks = jnp.max(
        jnp.where(on_mine[:, None] & (rank[:, None] == numbers), number[:, None], 0), axis=0
    )
    info = jnp.concatenate([chip, rank, picks, (my_row % 2)[None], (my_row // 2)[None]]).astype(jnp.int32)
    at = 2 * window
    me = at + 2 * held

    index = owner * held + slot
    rows, lanes = row_pieces(matel, pick(info, matel, other, 0, at, me), my_row, my_col, depth, n_ga, n_gp)
    sources = spread(lanes, n_ga)
    labels = jnp.arange(n_ga * held, dtype=jnp.int32)
    level = jnp.sum(jnp.where(labels[None, :] == index[:, None], band_energy[None, :], 0.0), axis=1)
    detuning = energies[:, None] - level[None, :]
    blocks = cols // tile_width(cols, 1792)
    early = max(1, blocks // 7)
    middle = (blocks - early) // 2
    halves = []
    for number, piece in enumerate(((0, early), (early, middle), (early + middle, blocks - early - middle))):
        halves.append(fold(index, detuning * detuning, rows, pole_amp, pole_freq, piece))
    reach = n_ga // 2 - 1
    total = close(info, halves, sources, reach, 0, at, me)
    for more in range(1, held):
        def further(total):
            sources = spread(pick(info, matel, other, 2 * more, at, me), n_ga)
            return total + close(info, halves, sources, reach, 2 * more, at, me)

        total = lax.cond(jnp.max(rank) >= 2 * more, further, lambda total: total, total)

    total = gather_sum(total, "ga", n_ga, 1, 1)
    total = gather_sum(total, "ga", n_ga, 2, n_ga)
    total = gather_sum(total, "gp", n_gp, 1, n_gp)
    return total.reshape(energies.shape[0], states, states)


def solution(mesh):
    n_ga, n_gp = mesh.shape["ga"], mesh.shape["gp"]

    def body(*values):
        return shards(*values, n_ga=n_ga, n_gp=n_gp)

    return jax.shard_map(
        body,
        mesh=mesh,
        in_specs=(P("ga", None, "gp"), P("ga", "gp"), P("ga", "gp"), P(), P(), P(), P()),
        out_specs=P(),
        check_vma=False,
    )
```

```python
import functools

import jax
import jax.numpy as jnp
from jax import lax
from jax.experimental import pallas as pl
from jax.experimental.pallas import tpu as pltpu
from jax.sharding import PartitionSpec as P


FOLD_FLOPS = 48 * 10**9


def flip(values, axis, size, bit):
    return lax.ppermute(values, axis, [(i, i ^ bit) for i in range(size)])


def gather_sum(total, axis, size, bit, stop):
    while bit < size and bit <= stop:
        if 2 * bit < size and 2 * bit <= stop:
            parts = [flip(total, axis, size, mask) for mask in (bit, 2 * bit, 3 * bit)]
            total = (total + parts[0]) + (parts[1] + parts[2])
            bit *= 4
        else:
            total = total + flip(total, axis, size, bit)
            bit *= 2
    return total


def tile_width(cols, most):
    best = 128
    for count in range(1, most // 128 + 1):
        if cols % (128 * count) == 0:
            best = 128 * count
    return best


def fold_kernel(index_ref, detuning_ref, rows_ref, amp_ref, freq_ref, out_ref, *, inner):
    bands = out_ref.shape[0]
    states = rows_ref.shape[1]
    energies = out_ref.shape[1] // states

    def step(tile, carry):
        columns = pl.ds(pl.multiple_of(tile * inner, inner), inner)
        frequency = freq_ref[:, columns].astype(jnp.float32)
        numerator = amp_ref[:, columns].astype(jnp.float32) * frequency
        squared = frequency * frequency
        for band in range(bands):
            rows = rows_ref[index_ref[band]]
            for energy in range(energies):
                pole = numerator / (squared + detuning_ref[energy, band])
                folded = jnp.dot(rows, pole.astype(jnp.bfloat16), preferred_element_type=jnp.float32)
                out_ref[band, energy * states:(energy + 1) * states, columns] = folded.astype(jnp.bfloat16)
        return carry

    lax.fori_loop(0, amp_ref.shape[1] // inner, step, 0)


def fold(index, detuning_squared, rows, amp, freq, piece):
    stored, states, depth = rows.shape
    energies, bands = detuning_squared.shape
    width = tile_width(amp.shape[1], 1792)
    first, steps = piece
    cols = steps * width
    inner = tile_width(width, 1792)
    return pl.pallas_call(
        functools.partial(fold_kernel, inner=inner),
        grid=(steps,),
        in_specs=[
            pl.BlockSpec(memory_space=pltpu.SMEM),
            pl.BlockSpec(memory_space=pltpu.SMEM),
            pl.BlockSpec((stored, states, depth), lambda i: (0, 0, 0)),
            pl.BlockSpec((depth, width), lambda i: (0, i + first)),
            pl.BlockSpec((depth, width), lambda i: (0, i + first)),
        ],
        out_specs=pl.BlockSpec((bands, energies * states, width), lambda i: (0, 0, i)),
        out_shape=jax.ShapeDtypeStruct((bands, energies * states, cols), jnp.bfloat16),
        compiler_params=pltpu.CompilerParams(vmem_limit_bytes=60 * 2**20),
        cost_estimate=pl.CostEstimate(
            flops=FOLD_FLOPS * cols // amp.shape[1], bytes_accessed=2 * depth * cols, transcendentals=0
        ),
        name="fold",
    )(index, detuning_squared, rows, amp, freq)


def pick_kernel(info_ref, mine_ref, other_ref, first_ref, second_ref, sems, *, base, at, me):
    held = mine_ref.shape[0]
    core = info_ref[me]
    for lane, out_ref in enumerate((first_ref, second_ref)):
        band = info_ref[at + base + lane]
        place = lax.rem(band, held)

        @pl.when(lax.div(band, held) == core)
        def _():
            pltpu.make_async_copy(mine_ref.at[place], out_ref, sems.at[lane]).start()

        @pl.when(lax.div(band, held) != core)
        def _():
            pltpu.make_async_copy(other_ref.at[place], out_ref, sems.at[lane]).start()

    for lane, out_ref in enumerate((first_ref, second_ref)):
        pltpu.make_async_copy(mine_ref.at[0], out_ref, sems.at[lane]).wait()


def pick(info, mine, other, base, at, me):
    shape = jax.ShapeDtypeStruct(mine.shape[1:], mine.dtype)
    return pl.pallas_call(
        functools.partial(pick_kernel, base=base, at=at, me=me),
        in_specs=[
            pl.BlockSpec(memory_space=pltpu.SMEM),
            pl.BlockSpec(memory_space=pltpu.HBM),
            pl.BlockSpec(memory_space=pltpu.HBM),
        ],
        out_specs=[pl.BlockSpec(memory_space=pltpu.VMEM)] * 2,
        out_shape=[shape, shape],
        scratch_shapes=[pltpu.SemaphoreType.DMA((2,))],
        compiler_params=pltpu.CompilerParams(vmem_limit_bytes=60 * 2**20),
        name="pick",
    )(info, mine, other)


def close_kernel(info_ref, *refs, window, pieces, reach, unit, base, at, me):
    halves = refs[:pieces]
    sources = refs[pieces:pieces + 2 + 4 * reach]
    out_ref, half_buf, column_buf, half_sems, column_sems = refs[pieces + 2 + 4 * reach:]
    core = info_ref[me]
    place = info_ref[me + 1]
    sign = 1 - 2 * core
    for band in range(window):
        apart = info_ref[band] - place
        lane = info_ref[window + band] - base
        for which in range(2):
            table = [(sources[which], 0)]
            for hop in range(1, reach + 1):
                table.append((sources[2 + 4 * (hop - 1) + which], sign * hop))
                table.append((sources[4 + 4 * (hop - 1) + which], -sign * hop))
            for ref, distance in table:
                @pl.when((lane == which) & (apart == distance))
                def _():
                    pltpu.make_async_copy(ref, column_buf.at[band], column_sems.at[band]).start()

    width = unit
    starts = []
    for half in halves:
        for part in range(half.shape[2] // width):
            place_in = pl.ds(part * width, width)
            pltpu.make_async_copy(half.at[:, :, place_in], half_buf.at[len(starts)], half_sems.at[len(starts)]).start()
            starts.append(part)
    for band in range(window):
        lane = info_ref[window + band] - base
        live = (lane >= 0) & (lane < 2)

        @pl.when(live)
        def _():
            pltpu.make_async_copy(sources[0], column_buf.at[band], column_sems.at[band]).wait()

        @pl.when(jnp.logical_not(live))
        def _():
            column_buf[band] = jnp.zeros_like(column_buf[band])

    def step(piece, total):
        pltpu.make_async_copy(halves[0].at[:, :, pl.ds(0, width)], half_buf.at[piece], half_sems.at[piece]).wait()
        columns = pl.ds(pl.multiple_of(piece * width, 128), width)
        for band in range(window):
            total += lax.dot_general(
                half_buf[piece, band], column_buf[band, :, columns], (((1,), (1,)), ((), ())),
                preferred_element_type=jnp.float32,
            )
        return total

    out_ref[...] = lax.fori_loop(0, len(starts), step, jnp.zeros(out_ref.shape, jnp.float32))


def close(info, halves, sources, reach, base, at, me):
    bands, pairs = halves[0].shape[:2]
    states, cols = sources[0].shape
    pieces = len(halves)
    unit = tile_width(cols, 1792)
    hbm = pl.BlockSpec(memory_space=pltpu.HBM)
    return pl.pallas_call(
        functools.partial(
            close_kernel, window=bands, pieces=pieces, reach=reach, unit=unit, base=base, at=at, me=me
        ),
        in_specs=[pl.BlockSpec(memory_space=pltpu.SMEM)] + [hbm] * (pieces + len(sources)),
        out_specs=pl.BlockSpec(memory_space=pltpu.VMEM),
        out_shape=jax.ShapeDtypeStruct((pairs, states), jnp.float32),
        scratch_shapes=[
            pltpu.VMEM((cols // unit, bands, pairs, unit), jnp.bfloat16),
            pltpu.VMEM((bands, states, cols), jnp.bfloat16),
            pltpu.SemaphoreType.DMA((cols // unit,)),
            pltpu.SemaphoreType.DMA((bands,)),
        ],
        compiler_params=pltpu.CompilerParams(vmem_limit_bytes=60 * 2**20),
        name="close",
    )(info, *halves, *sources)


def spread(lanes, n_ga):
    line = [(i + 1, i + 3) for i in range(0, n_ga - 2, 2)] + [(i + 2, i) for i in range(0, n_ga - 2, 2)]
    lanes = list(lanes)
    sources = list(lanes)
    for _ in range(1, n_ga // 2):
        hopped = []
        for lane in lanes:
            hopped.append(lax.ppermute(lane, "ga", line))
        lanes = hopped
        sources += lanes
        for lane in lanes:
            sources.append(flip(lane, "ga", n_ga, 1))
    return sources


def row_pieces(matel, lanes, my_row, my_col, depth, n_ga, n_gp):
    held, states, cols = matel.shape
    local = min(cols, n_ga * depth)
    per_block = cols // depth
    pieces = matel[:, :, :local].reshape(held, states, local // depth, depth)
    pieces = jnp.moveaxis(pieces, 2, 0)
    if local < n_ga * depth:
        spare = jnp.zeros((n_ga - local // depth,) + pieces.shape[1:], pieces.dtype)
        pieces = jnp.concatenate([pieces, spare])
        pieces = jnp.roll(pieces, my_col * per_block, axis=0)
    pieces = pieces.reshape((n_ga // 2, 2) + pieces.shape[1:])
    upper = my_row % 2 != 0
    got = flip(jnp.where(upper, pieces[:, 0], pieces[:, 1]), "ga", n_ga, 1)
    keep = jnp.where(upper, pieces[:, 1], pieces[:, 0])
    pieces = jnp.stack([jnp.where(upper, got, keep), jnp.where(upper, keep, got)], axis=1)
    bit = n_ga // 2
    while bit > 1:
        upper = (my_row & bit) != 0
        half = pieces.shape[0] // 2
        keep = jnp.where(upper, pieces[half:], pieces[:half])
        send = jnp.where(upper, pieces[:half], pieces[half:])
        got = flip(send, "ga", n_ga, bit)
        pieces = jnp.where(
            upper, jnp.concatenate([got, keep], axis=1), jnp.concatenate([keep, got], axis=1)
        )
        bit //= 2
    pieces, lanes = lax.optimization_barrier((pieces, lanes))
    bits = n_ga.bit_length() - 1
    order = pieces[0].reshape((2,) * bits + pieces.shape[2:])
    order = jnp.transpose(order, tuple(reversed(range(bits - 1))) + tuple(range(bits - 1, order.ndim)))
    order = order.reshape((n_ga * held, states, depth))
    here = my_col == (my_row * depth) // cols
    rows = jnp.where(here, order, jnp.zeros((), matel.dtype))
    bit = 1
    while bit < n_gp:
        rows = rows + flip(rows, "gp", n_gp, bit)
        bit *= 2
    return rows, lanes


def shards(matel, pole_amp, pole_freq, band_energy, energies, owner, slot, *, n_ga, n_gp):
    held, states, cols = matel.shape
    depth = pole_amp.shape[0]
    window = owner.shape[0]
    my_row = lax.axis_index("ga")
    my_col = lax.axis_index("gp")
    other = flip(matel, "ga", n_ga, 1)

    chip = owner // 2
    number = (owner % 2) * held + slot
    numbers = jnp.arange(2 * held, dtype=jnp.int32)
    wanted = jnp.any(
        (chip[:, None, None] == chip[None, :, None]) & (number[None, :, None] == numbers), axis=1
    )
    rank = jnp.sum(wanted & (numbers < number[:, None]), axis=1, dtype=jnp.int32)
    on_mine = chip == my_row // 2
    picks = jnp.max(
        jnp.where(on_mine[:, None] & (rank[:, None] == numbers), number[:, None], 0), axis=0
    )
    info = jnp.concatenate([chip, rank, picks, (my_row % 2)[None], (my_row // 2)[None]]).astype(jnp.int32)
    at = 2 * window
    me = at + 2 * held

    index = owner * held + slot
    rows, lanes = row_pieces(matel, pick(info, matel, other, 0, at, me), my_row, my_col, depth, n_ga, n_gp)
    sources = spread(lanes, n_ga)
    labels = jnp.arange(n_ga * held, dtype=jnp.int32)
    level = jnp.sum(jnp.where(labels[None, :] == index[:, None], band_energy[None, :], 0.0), axis=1)
    detuning = energies[:, None] - level[None, :]
    blocks = cols // tile_width(cols, 1792)
    early = max(1, blocks // 7)
    middle = max(1, (blocks - early) * 5 // 12)
    halves = []
    for number, piece in enumerate(((0, early), (early, middle), (early + middle, blocks - early - middle))):
        halves.append(fold(index, detuning * detuning, rows, pole_amp, pole_freq, piece))
    reach = n_ga // 2 - 1
    total = close(info, halves, sources, reach, 0, at, me)
    for more in range(1, held):
        def further(total):
            sources = spread(pick(info, matel, other, 2 * more, at, me), n_ga)
            return total + close(info, halves, sources, reach, 2 * more, at, me)

        total = lax.cond(jnp.max(rank) >= 2 * more, further, lambda total: total, total)

    total = gather_sum(total, "ga", n_ga, 1, 1)
    total = gather_sum(total, "ga", n_ga, 2, n_ga)
    total = gather_sum(total, "gp", n_gp, 1, n_gp)
    return total.reshape(energies.shape[0], states, states)


def solution(mesh):
    n_ga, n_gp = mesh.shape["ga"], mesh.shape["gp"]

    def body(*values):
        return shards(*values, n_ga=n_ga, n_gp=n_gp)

    return jax.shard_map(
        body,
        mesh=mesh,
        in_specs=(P("ga", None, "gp"), P("ga", "gp"), P("ga", "gp"), P(), P(), P(), P()),
        out_specs=P(),
        check_vma=False,
    )
```
